32 devices in a mesh: scen: 8 (over z, x), blk: 4 (over y, core).
Axes of the slice: x: 2, y: 2, z: 4, core: 2. Of those that a mesh axis runs over, the one named last changes fastest.
Arguments:
- cons_matrix: bfloat16 [2048, 4096], P(None, 'blk'), may hold values from -0.09375 to 0.09375
- row_scale: float32 [512, 2048], P('scen'), may hold values from 0.5 to 2
- rhs: float32 [512, 2048], P('scen'), may hold values from -6 to 6
- cons_mult: float32 [512, 2048], P('scen'), may hold values from -3 to 3
- cost: float32 [512, 4096], P('scen', 'blk'), may hold values from -6 to 6
- ph_mult: float32 [512, 4096], P('scen', 'blk'), may hold values from -3 to 3
- start: float32 [512, 4096], P('scen', 'blk'), may hold values from -3 to 3
- consensus: float32 [4096], P('blk'), may hold values from -3 to 3
- upper: float32 [4096], P('blk'), may hold values from 0.3 to 1.5
- prob: float32 [512], P('scen'), may hold values from 1 to 30, as said below
Outputs:
- solutions: float32 [512, 4096], P('scen', 'blk')
- mult_new: float32 [512, 2048], P('scen', 'blk')
- z_new: float32 [4096], P('blk')
- w_new: float32 [512, 4096], P('scen', 'blk')
- primal_res: float32 [], replicated
- dual_res: float32 [], replicated
The draws below stay inside these ranges and needn't reach their ends.
Inputs may be any that keep to these rules, and one draw needn't show every extreme that they name: prob is positive.
All inputs are finite; a program needn't handle non-finite values.
Results may differ from the reference program's by a relative error of at most 0.0017.
Values may be sent and summed in bfloat16 or wider, within the bound.
A program may use at most 64 MiB of HBM per device.

```python
import math
import jax
import jax.numpy as jnp
from jax import lax

M = 2048
NV = 4096
ITERS = 8
SCEN = 512


def draw_prob(key, part):
    index = jnp.arange(SCEN).astype(jnp.float32)
    base = jnp.exp(jnp.log(3.0) * index / max(SCEN - 1, 1))
    noise = jax.random.uniform(key, (SCEN,), jnp.float32, 1.0, 3.0)
    return (base * noise).astype(jnp.float32)


def steps_of(stream_key, dims, cuts, low, largest):
    def one(dim, shards_of):
        steps = jax.random.uniform(jax.random.fold_in(jax.random.fold_in(stream_key, 6), dim), (shards_of,), jnp.float32, low / len(cuts), largest / len(cuts))
        return jnp.repeat(jnp.exp(steps), dims[dim] // shards_of).reshape((-1,) + (1,) * (len(dims) - dim - 1))

    factor_of = one(*cuts[0])
    for cut in cuts[1:]:
        factor_of = factor_of * one(*cut)
    return factor_of


def gaussian(own_key, extent, scale, bound, cuts=(), dtype=jnp.bfloat16):
    result = jax.random.normal(own_key, extent, jnp.float32) * scale
    if len(cuts) > 0:
        result = steps_of(own_key, extent, cuts, -0.22, 0.18) * result
    return jnp.clip(result, min=-bound, max=bound).astype(dtype)


def setup_inputs(seed: int = 0) -> dict:
    seeds = jax.random.split(jax.random.key(seed), 11)
    cons_matrix = gaussian(seeds[0], (M, NV), NV ** -0.5, 0.09375, ((1, 4),))
    row_scale = jnp.clip(jnp.exp(math.log(2.0) - 1.3862944 * jax.random.uniform(seeds[1], (SCEN, M), jnp.float32) ** steps_of(seeds[1], (SCEN, M), ((0, 8),), -0.2, 0.2)), 0.5, 2.0)
    rhs = gaussian(seeds[2], (SCEN, M), 1.0, 6.0, ((0, 8),), jnp.float32)
    cons_mult = gaussian(seeds[3], (SCEN, M), 0.5, 3.0, ((0, 8),), jnp.float32)
    cost = gaussian(seeds[4], (SCEN, NV), 1.0, 6.0, ((0, 8), (1, 4)), jnp.float32)
    ph_mult = gaussian(seeds[5], (SCEN, NV), 0.5, 3.0, ((0, 8), (1, 4)), jnp.float32)
    start = gaussian(seeds[6], (SCEN, NV), 0.5, 3.0, ((0, 8), (1, 4)), jnp.float32)
    consensus = gaussian(seeds[7], (NV,), 0.5, 3.0, ((0, 4),), jnp.float32)
    upper = jnp.clip(0.3 + 1.2 * jax.random.uniform(seeds[8], (NV,), jnp.float32) ** steps_of(seeds[8], (NV,), ((0, 4),), -0.2, 0.2), 0.3, 1.5)
    prob = draw_prob(jax.random.fold_in(seeds[10], 71), 0)
    return dict(cons_matrix=cons_matrix, row_scale=row_scale, rhs=rhs, cons_mult=cons_mult, cost=cost, ph_mult=ph_mult, start=start, consensus=consensus, upper=upper, prob=prob)


penalty = 1.0
aug_weight = 1.0
step_size = 0.05
eps = 1e-06

def reference(cons_matrix, row_scale, rhs, cons_mult, cost, ph_mult, start, consensus, upper, prob):
    x_now = start
    for step in range(ITERS):
        prod = jnp.dot(x_now.astype(jnp.bfloat16), cons_matrix.T, preferred_element_type=jnp.float32)
        weighted = (row_scale * (cons_mult + aug_weight * (row_scale * prod - rhs))).astype(jnp.bfloat16)
        back = jnp.dot(weighted, cons_matrix, preferred_element_type=jnp.float32)
        grad = cost + ph_mult + penalty * (x_now - consensus[None, :]) + back
        x_now = jnp.clip(x_now - step_size * grad, -upper[None, :], upper[None, :])
    prod_end = jnp.dot(x_now.astype(jnp.bfloat16), cons_matrix.T, preferred_element_type=jnp.float32)
    mult_new = cons_mult + aug_weight * (row_scale * prod_end - rhs)
    total = jnp.sum(prob)
    z_new = lax.optimization_barrier(jnp.sum(prob[:, None] * x_now, axis=0)) / total
    w_new = ph_mult + penalty * (x_now - z_new[None, :])
    primal_res = jnp.sqrt(jnp.sum(prob[:, None] * (x_now - z_new[None, :]) ** 2) / (total * NV) + eps)
    dual_res = penalty * jnp.sqrt(jnp.sum((z_new - consensus) ** 2) / NV + eps)
    return (x_now, mult_new, z_new, w_new, primal_res, dual_res)
```

```python
import functools

import jax
import jax.numpy as jnp
from jax import lax
from jax.experimental import pallas as pl
from jax.experimental.pallas import tpu as pltpu
from jax.sharding import PartitionSpec as P

ITERS = 8
MESH = pl.DeviceIdType.MESH

penalty = 1.0
aug_weight = 1.0
step_size = 0.05
eps = 1e-06


def kernel(
    n_blk, n_scen,
    a, row_scale, rhs, mult, cost, ph, start, consensus, upper, prob,
    sol_out, mult_out, z_out, w_out, primal_out, dual_out,
    a_v, at_v, scale_v, rhs_v, mult_v, sq_v, lin_v, cost_v, ph_v, ph_far, x_v, xb_v, base_v,
    cons_v, up_v, prob_v, p_v, acc_v, send_v, recv_v, end_v, x_far, m_send, m_far, sums_v, norms_v,
    local_sem, pair_send, pair_recv, y_send, y_recv, end_send, end_recv, s_send, s_recv, n_send, n_recv,
):
    n_red = n_blk // 2
    n_chunk, rows, nv = a_v.shape[1:]
    half = x_v.shape[1]
    b, s = lax.axis_index("blk"), lax.axis_index("scen")
    group, core = lax.div(b, 2), lax.rem(b, 2)
    partner = {"blk": b + 1 - 2 * core}
    own_rows = pl.ds(pl.multiple_of(core * half, half), half)
    far_rows = pl.ds(pl.multiple_of((1 - core) * half, half), half)

    def peer(j):
        return {"blk": lax.rem(group + j, n_red) * 2 + core}

    def scen_peer(j):
        return {"scen": lax.rem(s + j, n_scen)}

    def blk_peer(j):
        return {"blk": lax.rem(b + j, n_blk)}

    def remote(src, dst, send, recv, device):
        return pltpu.make_async_remote_copy(
            src_ref=src, dst_ref=dst, send_sem=send, recv_sem=recv, device_id=device, device_id_type=MESH
        )

    barrier = pltpu.get_barrier_semaphore()
    for j in range(1, n_blk):
        pl.semaphore_signal(barrier, inc=1, device_id=blk_peer(j), device_id_type=MESH)
    for j in range(1, n_scen):
        pl.semaphore_signal(barrier, inc=1, device_id=scen_peer(j), device_id_type=MESH)

    local = []

    def fetch(src, dst):
        copy = pltpu.make_async_copy(src, dst, local_sem.at[len(local)])
        copy.start()
        local.append(copy)

    for k in range(n_chunk):
        fetch(a.at[pl.ds(k * rows, rows), :], a_v.at[0, k])
    fetch(row_scale.at[own_rows, :], scale_v)
    fetch(rhs.at[own_rows, :], rhs_v)
    fetch(mult.at[own_rows, :], mult_v)
    fetch(cost.at[own_rows, :], cost_v.at[0])
    fetch(start.at[own_rows, :], x_v.at[0])
    fetch(ph, ph_v)
    fetch(consensus, cons_v.at[0])
    fetch(upper, up_v.at[0])
    fetch(prob, prob_v)

    pl.semaphore_wait(barrier, n_blk + n_scen - 2)

    pair = []

    def push(src, dst):
        n = len(pair)
        copy = remote(src, dst, pair_send.at[n], pair_recv.at[n], partner)
        copy.start()
        pair.append(copy)

    push(cost.at[far_rows, :], cost_v.at[1])
    push(ph.at[far_rows, :], ph_far)
    push(start.at[far_rows, :], x_v.at[1])
    push(consensus, cons_v.at[1])
    push(upper, up_v.at[1])
    for k in range(n_chunk):
        push(a.at[pl.ds(k * rows, rows), :], a_v.at[1, k])

    for k in range(n_chunk):
        local[k].wait()
        at_v[k, 0] = a_v[0, k].T
    for copy in local[n_chunk:]:
        copy.wait()
    for k in range(n_chunk):
        lanes = pl.ds(k * rows, rows)
        scale = scale_v[:, lanes]
        sq_v[k] = aug_weight * scale * scale
        lin_v[k] = scale * (mult_v[:, lanes] - aug_weight * rhs_v[:, lanes])
    base_v[0] = cost_v[0] + ph_v[own_rows, :] - penalty * cons_v[0]
    for copy in pair[:5]:
        copy.wait()
    base_v[1] = cost_v[1] + ph_far[...] - penalty * cons_v[1]
    xb_v[...] = x_v[...].astype(jnp.bfloat16)
    for k in range(n_chunk):
        pair[5 + k].wait()
        at_v[k, 1] = a_v[1, k].T

    def product(k):
        return jnp.dot(xb_v[0], at_v[k, 0], preferred_element_type=jnp.float32) + jnp.dot(
            xb_v[1], at_v[k, 1], preferred_element_type=jnp.float32
        )

    def step(t, carry):
        slot = lax.rem(t, 2)
        copies = []
        for k in range(n_chunk):
            p = product(k)
            p_v[k] = p
            send_v[slot, k] = p.astype(jnp.bfloat16)
            row = []
            for j in range(1, n_red):
                copy = remote(
                    send_v.at[slot, k], recv_v.at[slot, j - 1, k],
                    y_send.at[slot, j - 1, k], y_recv.at[slot, j - 1, k], peer(j),
                )
                copy.start()
                row.append(copy)
            copies.append(row)
        for k in range(n_chunk):
            total = p_v[k]
            for j in range(1, n_red):
                copies[k][j - 1].wait_recv()
                total = total + recv_v[slot, j - 1, k].astype(jnp.float32)
            weighted = (lin_v[k] + sq_v[k] * total).astype(jnp.bfloat16)
            for i in range(2):
                back = jnp.dot(weighted, a_v[i, k], preferred_element_type=jnp.float32)
                acc_v[i] = back if k == 0 else acc_v[i] + back
        for i in range(2):
            x = x_v[i]
            grad = base_v[i] + penalty * x + acc_v[i]
            box = up_v[i]
            x = jnp.clip(x - step_size * grad, -box, box)
            x_v[i] = x
            xb_v[i] = x.astype(jnp.bfloat16)
        for row in copies:
            for copy in row:
                copy.wait_send()
        return carry

    lax.fori_loop(0, ITERS, step, 0)

    n = len(pair)
    push(x_v.at[1], x_far)

    ends = []
    for j in range(1, n_red):
        other = lax.rem(group + j, n_red) * 2
        for i in range(2):
            p_v[other + i] = product(other + i)
            copy = remote(
                p_v.at[other + i], end_v.at[j - 1, i], end_send.at[j - 1, i], end_recv.at[j - 1, i], peer(j)
            )
            copy.start()
            ends.append(copy)

    square = prob_v.shape[1]
    diagonal = lax.broadcasted_iota(jnp.int32, (square, square), 0) == lax.broadcasted_iota(
        jnp.int32, (square, square), 1
    )
    prob_col = jnp.sum(jnp.where(diagonal, prob_v[...], 0.0), axis=1, keepdims=True)
    part_total = jnp.sum(prob_col, axis=0, keepdims=True)
    sol_out[own_rows, :] = x_v[0]
    pair[n].wait()
    sol_out[far_rows, :] = x_far[...]
    x_end = sol_out[...]
    part_sum = jnp.sum(prob_col * x_end, axis=0, keepdims=True)
    spread = jnp.sum(prob_col * (x_end - part_sum / part_total) ** 2, axis=0, keepdims=True)
    spread = jnp.sum(spread, axis=1, keepdims=True)
    sums_v[s, :, pl.ds(0, nv)] = part_sum
    sums_v[s, :, pl.ds(nv, 128)] = jnp.broadcast_to(part_total, (1, 128))
    sums_v[s, :, pl.ds(nv + 128, 128)] = jnp.broadcast_to(spread, (1, 128))
    gathers = []
    for j in range(1, n_scen):
        copy = remote(sums_v.at[s], sums_v.at[s], s_send.at[j - 1], s_recv.at[j - 1], scen_peer(j))
        copy.start()
        gathers.append(copy)

    for i in range(2):
        p_v[group * 2 + i] = product(group * 2 + i)
    for copy in ends:
        copy.wait()

    def new_mult(i):
        k = group * 2 + i
        total = p_v[k]
        for j in range(1, n_red):
            total = total + end_v[j - 1, i]
        lanes = pl.ds(pl.multiple_of(k * rows, rows), rows)
        return mult_v[:, lanes] + aug_weight * (scale_v[:, lanes] * total - rhs_v[:, lanes])

    m_send[...] = new_mult(1 - core)
    n = len(pair)
    push(m_send, m_far)
    mult_out[own_rows, :] = new_mult(core)

    for copy in gathers:
        copy.wait()
    total_sum = sums_v[0, :, pl.ds(0, nv)]
    total = sums_v[0, :, pl.ds(nv, 128)]
    primal = sums_v[0, :, pl.ds(nv + 128, 128)]
    for i in range(1, n_scen):
        total_sum = total_sum + sums_v[i, :, pl.ds(0, nv)]
        total = total + sums_v[i, :, pl.ds(nv, 128)]
        primal = primal + sums_v[i, :, pl.ds(nv + 128, 128)]
    z_new = total_sum / total[:, :1]
    between = jnp.zeros_like(z_new)
    for i in range(n_scen):
        weight = sums_v[i, :, pl.ds(nv, 128)][:, :1]
        between = between + weight * (sums_v[i, :, pl.ds(0, nv)] / weight - z_new) ** 2
    primal = primal + jnp.sum(between, axis=1, keepdims=True)
    dual = jnp.sum((z_new - cons_v[0]) ** 2, axis=1, keepdims=True)
    norms_v[b, :, pl.ds(0, 128)] = primal
    norms_v[b, :, pl.ds(128, 128)] = jnp.broadcast_to(dual, (1, 128))
    norms = []
    for j in range(1, n_blk):
        copy = remote(norms_v.at[b], norms_v.at[b], n_send.at[j - 1], n_recv.at[j - 1], blk_peer(j))
        copy.start()
        norms.append(copy)
    z_out[...] = z_new
    w_out[...] = ph_v[...] + penalty * (sol_out[...] - z_new)
    pair[n].wait()
    mult_out[far_rows, :] = m_far[...]
    for copy in norms:
        copy.wait()
    primal = norms_v[0, :, pl.ds(0, 128)]
    dual = norms_v[0, :, pl.ds(128, 128)]
    for i in range(1, n_blk):
        primal = primal + norms_v[i, :, pl.ds(0, 128)]
        dual = dual + norms_v[i, :, pl.ds(128, 128)]
    width = nv * n_blk
    primal_out[...] = jnp.sqrt(primal / (total * width) + eps)
    dual_out[...] = penalty * jnp.sqrt(dual / width + eps)


def solution(mesh):
    n_blk, n_scen = mesh.shape["blk"], mesh.shape["scen"]
    f32, bf16 = jnp.float32, jnp.bfloat16

    def per_device(cons_matrix, row_scale, rhs, cons_mult, cost, ph_mult, start, consensus, upper, prob):
        m, nv = cons_matrix.shape
        scen = cost.shape[0]
        half, rows = scen // 2, m // n_blk
        n_red = n_blk // 2
        any_spec = pl.BlockSpec(memory_space=pl.ANY)
        vmem = pl.BlockSpec(memory_space=pltpu.VMEM)
        dma = pltpu.SemaphoreType.DMA
        sol, mult_new, z_new, w_new, primal, dual = pl.pallas_call(
            functools.partial(kernel, n_blk, n_scen),
            out_shape=(
                jax.ShapeDtypeStruct((scen, nv), f32),
                jax.ShapeDtypeStruct((scen, rows), f32),
                jax.ShapeDtypeStruct((1, nv), f32),
                jax.ShapeDtypeStruct((scen, nv), f32),
                jax.ShapeDtypeStruct((1, 128), f32),
                jax.ShapeDtypeStruct((1, 128), f32),
            ),
            in_specs=[any_spec] * 10,
            out_specs=[vmem] * 6,
            scratch_shapes=[
                pltpu.VMEM((2, n_blk, rows, nv), bf16),
                pltpu.VMEM((n_blk, 2, nv, rows), bf16),
                pltpu.VMEM((half, m), f32),
                pltpu.VMEM((half, m), f32),
                pltpu.VMEM((half, m), f32),
                pltpu.VMEM((n_blk, half, rows), f32),
                pltpu.VMEM((n_blk, half, rows), f32),
                pltpu.VMEM((2, half, nv), f32),
                pltpu.VMEM((scen, nv), f32),
                pltpu.VMEM((half, nv), f32),
                pltpu.VMEM((2, half, nv), f32),
                pltpu.VMEM((2, half, nv), bf16),
                pltpu.VMEM((2, half, nv), f32),
                pltpu.VMEM((2, 1, nv), f32),
                pltpu.VMEM((2, 1, nv), f32),
                pltpu.VMEM((1, scen), f32),
                pltpu.VMEM((n_blk, half, rows), f32),
                pltpu.VMEM((2, half, nv), f32),
                pltpu.VMEM((2, n_blk, half, rows), bf16),
                pltpu.VMEM((2, n_red - 1, n_blk, half, rows), bf16),
                pltpu.VMEM((n_red - 1, 2, half, rows), f32),
                pltpu.VMEM((half, nv), f32),
                pltpu.VMEM((half, rows), f32),
                pltpu.VMEM((half, rows), f32),
                pltpu.VMEM((n_scen, 1, nv + 256), f32),
                pltpu.VMEM((n_blk, 1, 256), f32),
                dma((n_blk + 9,)),
                dma((n_blk + 7,)),
                dma((n_blk + 7,)),
                dma((2, n_red - 1, n_blk)),
                dma((2, n_red - 1, n_blk)),
                dma((n_red - 1, 2)),
                dma((n_red - 1, 2)),
                dma((n_scen - 1,)),
                dma((n_scen - 1,)),
                dma((n_blk - 1,)),
                dma((n_blk - 1,)),
            ],
            compiler_params=pltpu.CompilerParams(
                collective_id=0, has_side_effects=True, vmem_limit_bytes=48 * 1024 * 1024
            ),
        )(
            cons_matrix, row_scale, rhs, cons_mult, cost, ph_mult, start,
            consensus[None, :], upper[None, :], prob[None, :],
        )
        return sol, mult_new, z_new[0], w_new, primal[0, 0], dual[0, 0]

    in_specs = (
        P(None, "blk"),
        P("scen", None),
        P("scen", None),
        P("scen", None),
        P("scen", "blk"),
        P("scen", "blk"),
        P("scen", "blk"),
        P("blk"),
        P("blk"),
        P("scen"),
    )
    out_specs = (P("scen", "blk"), P("scen", "blk"), P("blk"), P("scen", "blk"), P(), P())
    return jax.shard_map(per_device, mesh=mesh, in_specs=in_specs, out_specs=out_specs, check_vma=False)
```

```python
import functools

import jax
import jax.numpy as jnp
from jax import lax
from jax.experimental import pallas as pl
from jax.experimental.pallas import tpu as pltpu
from jax.sharding import PartitionSpec as P

ITERS = 8
MESH = pl.DeviceIdType.MESH

penalty = 1.0
aug_weight = 1.0
step_size = 0.05
eps = 1e-06


def kernel(
    n_blk, n_scen,
    a, row_scale, rhs, mult, cost, ph, start, consensus, upper, prob,
    sol_out, mult_out, z_out, primal_out, dual_out,
    a_v, at_v, scale_v, rhs_v, mult_v, sq_v, lin_v, cost_v, ph_v, ph_far, x_v, xb_v, base_v,
    cons_v, up_v, prob_v, p_v, acc_v, send_v, recv_v, end_v, x_far, m_send, m_far, sums_v, norms_v,
    local_sem, pair_send, pair_recv, y_send, y_recv, end_send, end_recv, s_send, s_recv, n_send, n_recv,
):
    n_red = n_blk // 2
    n_chunk, rows, nv = a_v.shape[1:]
    half = x_v.shape[1]
    b, s = lax.axis_index("blk"), lax.axis_index("scen")
    group, core = lax.div(b, 2), lax.rem(b, 2)
    partner = {"blk": b + 1 - 2 * core}
    own_rows = pl.ds(pl.multiple_of(core * half, half), half)
    far_rows = pl.ds(pl.multiple_of((1 - core) * half, half), half)

    def peer(j):
        return {"blk": lax.rem(group + j, n_red) * 2 + core}

    def scen_peer(j):
        return {"scen": lax.rem(s + j, n_scen)}

    def blk_peer(j):
        return {"blk": lax.rem(b + j, n_blk)}

    def remote(src, dst, send, recv, device):
        return pltpu.make_async_remote_copy(
            src_ref=src, dst_ref=dst, send_sem=send, recv_sem=recv, device_id=device, device_id_type=MESH
        )

    barrier = pltpu.get_barrier_semaphore()
    for j in range(1, n_blk):
        pl.semaphore_signal(barrier, inc=1, device_id=blk_peer(j), device_id_type=MESH)
    for j in range(1, n_scen):
        pl.semaphore_signal(barrier, inc=1, device_id=scen_peer(j), device_id_type=MESH)

    local = []

    def fetch(src, dst):
        copy = pltpu.make_async_copy(src, dst, local_sem.at[len(local)])
        copy.start()
        local.append(copy)

    for k in range(n_chunk):
        fetch(a.at[pl.ds(k * rows, rows), :], a_v.at[0, k])
    fetch(row_scale.at[own_rows, :], scale_v)
    fetch(rhs.at[own_rows, :], rhs_v)
    fetch(mult.at[own_rows, :], mult_v)
    fetch(cost.at[own_rows, :], cost_v.at[0])
    fetch(start.at[own_rows, :], x_v.at[0])
    fetch(ph, ph_v)
    fetch(consensus, cons_v.at[0])
    fetch(upper, up_v.at[0])
    fetch(prob, prob_v)

    pl.semaphore_wait(barrier, n_blk + n_scen - 2)

    pair = []

    def push(src, dst):
        n = len(pair)
        copy = remote(src, dst, pair_send.at[n], pair_recv.at[n], partner)
        copy.start()
        pair.append(copy)

    push(cost.at[far_rows, :], cost_v.at[1])
    push(ph.at[far_rows, :], ph_far)
    push(start.at[far_rows, :], x_v.at[1])
    push(consensus, cons_v.at[1])
    push(upper, up_v.at[1])
    for k in range(n_chunk):
        push(a.at[pl.ds(k * rows, rows), :], a_v.at[1, k])

    for k in range(n_chunk):
        local[k].wait()
        at_v[k, 0] = a_v[0, k].T
    for copy in local[n_chunk:]:
        copy.wait()
    for k in range(n_chunk):
        lanes = pl.ds(k * rows, rows)
        scale = scale_v[:, lanes]
        sq_v[k] = aug_weight * scale * scale
        lin_v[k] = scale * (mult_v[:, lanes] - aug_weight * rhs_v[:, lanes])
    base_v[0] = cost_v[0] + ph_v[own_rows, :] - penalty * cons_v[0]
    for copy in pair[:5]:
        copy.wait()
    base_v[1] = cost_v[1] + ph_far[...] - penalty * cons_v[1]
    xb_v[...] = x_v[...].astype(jnp.bfloat16)
    for k in range(n_chunk):
        pair[5 + k].wait()
        at_v[k, 1] = a_v[1, k].T

    def product(k):
        return jnp.dot(xb_v[0], at_v[k, 0], preferred_element_type=jnp.float32) + jnp.dot(
            xb_v[1], at_v[k, 1], preferred_element_type=jnp.float32
        )

    def step(t, carry):
        slot = lax.rem(t, 2)
        copies = []
        for k in range(n_chunk):
            p = product(k)
            p_v[k] = p
            send_v[slot, k] = p.astype(jnp.bfloat16)
            row = []
            for j in range(1, n_red):
                copy = remote(
                    send_v.at[slot, k], recv_v.at[slot, j - 1, k],
                    y_send.at[slot, j - 1, k], y_recv.at[slot, j - 1, k], peer(j),
                )
                copy.start()
                row.append(copy)
            copies.append(row)
        for k in range(n_chunk):
            total = p_v[k]
            for j in range(1, n_red):
                copies[k][j - 1].wait_recv()
                total = total + recv_v[slot, j - 1, k].astype(jnp.float32)
            weighted = (lin_v[k] + sq_v[k] * total).astype(jnp.bfloat16)
            for i in range(2):
                back = jnp.dot(weighted, a_v[i, k], preferred_element_type=jnp.float32)
                acc_v[i] = back if k == 0 else acc_v[i] + back
        for i in range(2):
            x = x_v[i]
            grad = base_v[i] + penalty * x + acc_v[i]
            box = up_v[i]
            x = jnp.clip(x - step_size * grad, -box, box)
            x_v[i] = x
            xb_v[i] = x.astype(jnp.bfloat16)
        for row in copies:
            for copy in row:
                copy.wait_send()
        return carry

    lax.fori_loop(0, ITERS, step, 0)

    n = len(pair)
    push(x_v.at[1], x_far)

    ends = []
    for j in range(1, n_red):
        other = lax.rem(group + j, n_red) * 2
        for i in range(2):
            p_v[other + i] = product(other + i)
            copy = remote(
                p_v.at[other + i], end_v.at[j - 1, i], end_send.at[j - 1, i], end_recv.at[j - 1, i], peer(j)
            )
            copy.start()
            ends.append(copy)

    square = prob_v.shape[1]
    diagonal = lax.broadcasted_iota(jnp.int32, (square, square), 0) == lax.broadcasted_iota(
        jnp.int32, (square, square), 1
    )
    prob_col = jnp.sum(jnp.where(diagonal, prob_v[...], 0.0), axis=1, keepdims=True)
    part_total = jnp.sum(prob_col, axis=0, keepdims=True)
    sol_out[own_rows, :] = x_v[0]
    pair[n].wait()
    sol_out[far_rows, :] = x_far[...]
    x_end = sol_out[...]
    part_sum = jnp.sum(prob_col * x_end, axis=0, keepdims=True)
    spread = jnp.sum(prob_col * (x_end - part_sum / part_total) ** 2, axis=0, keepdims=True)
    spread = jnp.sum(spread, axis=1, keepdims=True)
    sums_v[s, :, pl.ds(0, nv)] = part_sum
    sums_v[s, :, pl.ds(nv, 128)] = jnp.broadcast_to(part_total, (1, 128))
    sums_v[s, :, pl.ds(nv + 128, 128)] = jnp.broadcast_to(spread, (1, 128))
    gathers = []
    for j in range(1, n_scen):
        copy = remote(sums_v.at[s], sums_v.at[s], s_send.at[j - 1], s_recv.at[j - 1], scen_peer(j))
        copy.start()
        gathers.append(copy)

    for i in range(2):
        p_v[group * 2 + i] = product(group * 2 + i)
    for copy in ends:
        copy.wait()

    def new_mult(i):
        k = group * 2 + i
        total = p_v[k]
        for j in range(1, n_red):
            total = total + end_v[j - 1, i]
        lanes = pl.ds(pl.multiple_of(k * rows, rows), rows)
        return mult_v[:, lanes] + aug_weight * (scale_v[:, lanes] * total - rhs_v[:, lanes])

    m_send[...] = new_mult(1 - core)
    n = len(pair)
    push(m_send, m_far)
    mult_out[own_rows, :] = new_mult(core)

    for copy in gathers:
        copy.wait()
    total_sum = sums_v[0, :, pl.ds(0, nv)]
    total = sums_v[0, :, pl.ds(nv, 128)]
    primal = sums_v[0, :, pl.ds(nv + 128, 128)]
    for i in range(1, n_scen):
        total_sum = total_sum + sums_v[i, :, pl.ds(0, nv)]
        total = total + sums_v[i, :, pl.ds(nv, 128)]
        primal = primal + sums_v[i, :, pl.ds(nv + 128, 128)]
    z_new = total_sum / total[:, :1]
    between = jnp.zeros_like(z_new)
    for i in range(n_scen):
        weight = sums_v[i, :, pl.ds(nv, 128)][:, :1]
        between = between + weight * (sums_v[i, :, pl.ds(0, nv)] / weight - z_new) ** 2
    primal = primal + jnp.sum(between, axis=1, keepdims=True)
    dual = jnp.sum((z_new - cons_v[0]) ** 2, axis=1, keepdims=True)
    norms_v[b, :, pl.ds(0, 128)] = primal
    norms_v[b, :, pl.ds(128, 128)] = jnp.broadcast_to(dual, (1, 128))
    norms = []
    for j in range(1, n_blk):
        copy = remote(norms_v.at[b], norms_v.at[b], n_send.at[j - 1], n_recv.at[j - 1], blk_peer(j))
        copy.start()
        norms.append(copy)
    z_out[...] = z_new
    pair[n].wait()
    mult_out[far_rows, :] = m_far[...]
    for copy in norms:
        copy.wait()
    primal = norms_v[0, :, pl.ds(0, 128)]
    dual = norms_v[0, :, pl.ds(128, 128)]
    for i in range(1, n_blk):
        primal = primal + norms_v[i, :, pl.ds(0, 128)]
        dual = dual + norms_v[i, :, pl.ds(128, 128)]
    width = nv * n_blk
    primal_out[...] = jnp.sqrt(primal / (total * width) + eps)
    dual_out[...] = penalty * jnp.sqrt(dual / width + eps)


def finish(sol, mult, z, primal, dual, ph, sol_out, mult_out, z_out, w_out, primal_out, dual_out):
    sol_out[...] = sol[...]
    mult_out[...] = mult[...]
    z_out[...] = z[...]
    w_out[...] = ph[...] + penalty * (sol[...] - z[...])
    primal_out[...] = primal[...]
    dual_out[...] = dual[...]


def solution(mesh):
    n_blk, n_scen = mesh.shape["blk"], mesh.shape["scen"]
    f32, bf16 = jnp.float32, jnp.bfloat16

    def per_device(cons_matrix, row_scale, rhs, cons_mult, cost, ph_mult, start, consensus, upper, prob):
        m, nv = cons_matrix.shape
        scen = cost.shape[0]
        half, rows = scen // 2, m // n_blk
        n_red = n_blk // 2
        any_spec = pl.BlockSpec(memory_space=pl.ANY)
        vmem = pl.BlockSpec(memory_space=pltpu.VMEM)
        dma = pltpu.SemaphoreType.DMA
        ends = pl.pallas_call(
            functools.partial(kernel, n_blk, n_scen),
            out_shape=(
                jax.ShapeDtypeStruct((scen, nv), f32),
                jax.ShapeDtypeStruct((scen, rows), f32),
                jax.ShapeDtypeStruct((1, nv), f32),
                jax.ShapeDtypeStruct((1, 128), f32),
                jax.ShapeDtypeStruct((1, 128), f32),
            ),
            in_specs=[any_spec] * 10,
            out_specs=[vmem] * 5,
            scratch_shapes=[
                pltpu.VMEM((2, n_blk, rows, nv), bf16),
                pltpu.VMEM((n_blk, 2, nv, rows), bf16),
                pltpu.VMEM((half, m), f32),
                pltpu.VMEM((half, m), f32),
                pltpu.VMEM((half, m), f32),
                pltpu.VMEM((n_blk, half, rows), f32),
                pltpu.VMEM((n_blk, half, rows), f32),
                pltpu.VMEM((2, half, nv), f32),
                pltpu.VMEM((scen, nv), f32),
                pltpu.VMEM((half, nv), f32),
                pltpu.VMEM((2, half, nv), f32),
                pltpu.VMEM((2, half, nv), bf16),
                pltpu.VMEM((2, half, nv), f32),
                pltpu.VMEM((2, 1, nv), f32),
                pltpu.VMEM((2, 1, nv), f32),
                pltpu.VMEM((1, scen), f32),
                pltpu.VMEM((n_blk, half, rows), f32),
                pltpu.VMEM((2, half, nv), f32),
                pltpu.VMEM((2, n_blk, half, rows), bf16),
                pltpu.VMEM((2, n_red - 1, n_blk, half, rows), bf16),
                pltpu.VMEM((n_red - 1, 2, half, rows), f32),
                pltpu.VMEM((half, nv), f32),
                pltpu.VMEM((half, rows), f32),
                pltpu.VMEM((half, rows), f32),
                pltpu.VMEM((n_scen, 1, nv + 256), f32),
                pltpu.VMEM((n_blk, 1, 256), f32),
                dma((n_blk + 9,)),
                dma((n_blk + 7,)),
                dma((n_blk + 7,)),
                dma((2, n_red - 1, n_blk)),
                dma((2, n_red - 1, n_blk)),
                dma((n_red - 1, 2)),
                dma((n_red - 1, 2)),
                dma((n_scen - 1,)),
                dma((n_scen - 1,)),
                dma((n_blk - 1,)),
                dma((n_blk - 1,)),
            ],
            compiler_params=pltpu.CompilerParams(
                collective_id=0, has_side_effects=True, vmem_limit_bytes=67043328
            ),
        )(
            cons_matrix, row_scale, rhs, cons_mult, cost, ph_mult, start,
            consensus[None, :], upper[None, :], prob[None, :],
        )
        sol, mult_new, z_new, w_new, primal, dual = pl.pallas_call(
            finish,
            out_shape=tuple(
                jax.ShapeDtypeStruct(shape, f32)
                for shape in ((scen, nv), (scen, rows), (1, nv), (scen, nv), (1, 128), (1, 128))
            ),
            in_specs=[vmem] * 6,
            out_specs=[vmem] * 6,
        )(*ends, ph_mult)
        return sol, mult_new, z_new[0], w_new, primal[0, 0], dual[0, 0]

    in_specs = (
        P(None, "blk"),
        P("scen", None),
        P("scen", None),
        P("scen", None),
        P("scen", "blk"),
        P("scen", "blk"),
        P("scen", "blk"),
        P("blk"),
        P("blk"),
        P("scen"),
    )
    out_specs = (P("scen", "blk"), P("scen", "blk"), P("blk"), P("scen", "blk"), P(), P())
    return jax.shard_map(per_device, mesh=mesh, in_specs=in_specs, out_specs=out_specs, check_vma=False)
```

```python
import functools

import jax
import jax.numpy as jnp
from jax import lax
from jax.experimental import pallas as pl
from jax.experimental.pallas import tpu as pltpu
from jax.sharding import PartitionSpec as P

ITERS = 8
MESH = pl.DeviceIdType.MESH

penalty = 1.0
aug_weight = 1.0
step_size = 0.05
eps = 1e-06


def kernel(
    n_blk, n_scen,
    a, row_scale, rhs, mult, cost, ph, start, consensus, upper, prob,
    sol_out, mult_out, z_out, primal_out, dual_out,
    a_v, at_v, scale_v, rhs_v, mult_v, sq_v, lin_v, cost_v, ph_v, ph_far, x_v, xb_v, base_v,
    cons_v, up_v, prob_v, p_v, acc_v, send_v, recv_v, end_v, x_far, m_send, m_far, sums_v, norms_v, start_v, p_far, p_near,
    local_sem, pair_send, pair_recv, y_send, y_recv, end_send, end_recv, s_send, s_recv, n_send, n_recv,
):
    n_red = n_blk // 2
    n_chunk, rows, nv = a_v.shape[1:]
    half = x_v.shape[1]
    b, s = lax.axis_index("blk"), lax.axis_index("scen")
    group, core = lax.div(b, 2), lax.rem(b, 2)
    partner = {"blk": b + 1 - 2 * core}
    own_rows = pl.ds(pl.multiple_of(core * half, half), half)
    far_rows = pl.ds(pl.multiple_of((1 - core) * half, half), half)

    def peer(j):
        return {"blk": lax.rem(group + j, n_red) * 2 + core}

    def scen_peer(j):
        return {"scen": lax.rem(s + j, n_scen)}

    def blk_peer(j):
        return {"blk": lax.rem(b + j, n_blk)}

    def remote(src, dst, send, recv, device):
        return pltpu.make_async_remote_copy(
            src_ref=src, dst_ref=dst, send_sem=send, recv_sem=recv, device_id=device, device_id_type=MESH
        )

    barrier = pltpu.get_barrier_semaphore()
    for j in range(1, n_blk):
        pl.semaphore_signal(barrier, inc=1, device_id=blk_peer(j), device_id_type=MESH)
    for j in range(1, n_scen):
        pl.semaphore_signal(barrier, inc=1, device_id=scen_peer(j), device_id_type=MESH)

    local = []

    def fetch(src, dst):
        copy = pltpu.make_async_copy(src, dst, local_sem.at[len(local)])
        copy.start()
        local.append(copy)

    for k in range(n_chunk):
        fetch(a.at[pl.ds(k * rows, rows), :], a_v.at[0, k])
    fetch(row_scale.at[own_rows, :], scale_v)
    fetch(rhs.at[own_rows, :], rhs_v)
    fetch(mult.at[own_rows, :], mult_v)
    fetch(cost.at[own_rows, :], cost_v.at[0])
    fetch(start, start_v)
    fetch(ph, ph_v)
    fetch(consensus, cons_v.at[0])
    fetch(upper, up_v.at[0])
    fetch(prob, prob_v)

    for k in range(n_chunk):
        local[k].wait()
        at_v[k, 0] = a_v[0, k].T
    for copy in local[n_chunk:]:
        copy.wait()
    x_v[0] = start_v[own_rows, :]
    start_own = start_v[own_rows, :].astype(jnp.bfloat16)
    start_far = start_v[far_rows, :].astype(jnp.bfloat16)
    for k in range(n_chunk):
        p_far[k] = jnp.dot(start_far, at_v[k, 0], preferred_element_type=jnp.float32)
    for k in range(n_chunk):
        p_v[k] = jnp.dot(start_own, at_v[k, 0], preferred_element_type=jnp.float32)

    pl.semaphore_wait(barrier, n_blk + n_scen - 2)

    pair = []

    def push(src, dst):
        n = len(pair)
        copy = remote(src, dst, pair_send.at[n], pair_recv.at[n], partner)
        copy.start()
        pair.append(copy)

    for k in range(n_chunk):
        push(p_far.at[k], p_near.at[k])
    for k in range(n_chunk):
        push(a.at[pl.ds(k * rows, rows), :], a_v.at[1, k])
    push(cost.at[far_rows, :], cost_v.at[1])
    push(ph.at[far_rows, :], ph_far)
    push(start.at[far_rows, :], x_v.at[1])
    push(consensus, cons_v.at[1])
    push(upper, up_v.at[1])

    def product(k):
        return jnp.dot(xb_v[0], at_v[k, 0], preferred_element_type=jnp.float32) + jnp.dot(
            xb_v[1], at_v[k, 1], preferred_element_type=jnp.float32
        )

    def share(slot, k, p):
        p_v[k] = p
        send_v[slot, k] = p.astype(jnp.bfloat16)
        row = []
        for j in range(1, n_red):
            copy = remote(
                send_v.at[slot, k], recv_v.at[slot, j - 1, k],
                y_send.at[slot, j - 1, k], y_recv.at[slot, j - 1, k], peer(j),
            )
            copy.start()
            row.append(copy)
        return row

    def advance(slot, copies):
        for k in range(n_chunk):
            total = p_v[k]
            for j in range(1, n_red):
                copies[k][j - 1].wait_recv()
                total = total + recv_v[slot, j - 1, k].astype(jnp.float32)
            weighted = (lin_v[k] + sq_v[k] * total).astype(jnp.bfloat16)
            for i in range(2):
                back = jnp.dot(weighted, a_v[i, k], preferred_element_type=jnp.float32)
                acc_v[i] = back if k == 0 else acc_v[i] + back
        for i in range(2):
            x = x_v[i]
            grad = base_v[i] + penalty * x + acc_v[i]
            box = up_v[i]
            x = jnp.clip(x - step_size * grad, -box, box)
            x_v[i] = x
            xb_v[i] = x.astype(jnp.bfloat16)
        for row in copies:
            for copy in row:
                copy.wait_send()

    def step(t, carry):
        slot = lax.rem(t, 2)
        advance(slot, [share(slot, k, product(k)) for k in range(n_chunk)])
        return carry

    copies = []
    for k in range(n_chunk):
        pair[k].wait()
        copies.append(share(0, k, p_v[k] + p_near[k]))
    for k in range(n_chunk):
        lanes = pl.ds(k * rows, rows)
        scale = scale_v[:, lanes]
        sq_v[k] = aug_weight * scale * scale
        lin_v[k] = scale * (mult_v[:, lanes] - aug_weight * rhs_v[:, lanes])
    base_v[0] = cost_v[0] + ph_v[own_rows, :] - penalty * cons_v[0]
    for k in range(n_chunk):
        pair[n_chunk + k].wait()
        at_v[k, 1] = a_v[1, k].T
    for copy in pair[2 * n_chunk :]:
        copy.wait()
    base_v[1] = cost_v[1] + ph_far[...] - penalty * cons_v[1]
    advance(0, copies)

    lax.fori_loop(1, ITERS, step, 0)

    n = len(pair)
    push(x_v.at[1], x_far)

    ends = []
    for j in range(1, n_red):
        other = lax.rem(group + j, n_red) * 2
        for i in range(2):
            p_v[other + i] = product(other + i)
            copy = remote(
                p_v.at[other + i], end_v.at[j - 1, i], end_send.at[j - 1, i], end_recv.at[j - 1, i], peer(j)
            )
            copy.start()
            ends.append(copy)

    square = prob_v.shape[1]
    diagonal = lax.broadcasted_iota(jnp.int32, (square, square), 0) == lax.broadcasted_iota(
        jnp.int32, (square, square), 1
    )
    prob_col = jnp.sum(jnp.where(diagonal, prob_v[...], 0.0), axis=1, keepdims=True)
    part_total = jnp.sum(prob_col, axis=0, keepdims=True)
    sol_out[own_rows, :] = x_v[0]
    pair[n].wait()
    sol_out[far_rows, :] = x_far[...]
    x_end = sol_out[...]
    part_sum = jnp.sum(prob_col * x_end, axis=0, keepdims=True)
    spread = jnp.sum(prob_col * (x_end - part_sum / part_total) ** 2, axis=0, keepdims=True)
    spread = jnp.sum(spread, axis=1, keepdims=True)
    sums_v[s, :, pl.ds(0, nv)] = part_sum
    sums_v[s, :, pl.ds(nv, 128)] = jnp.broadcast_to(part_total, (1, 128))
    sums_v[s, :, pl.ds(nv + 128, 128)] = jnp.broadcast_to(spread, (1, 128))
    gathers = []
    for j in range(1, n_scen):
        copy = remote(sums_v.at[s], sums_v.at[s], s_send.at[j - 1], s_recv.at[j - 1], scen_peer(j))
        copy.start()
        gathers.append(copy)

    for i in range(2):
        p_v[group * 2 + i] = product(group * 2 + i)
    for copy in ends:
        copy.wait()

    def new_mult(i):
        k = group * 2 + i
        total = p_v[k]
        for j in range(1, n_red):
            total = total + end_v[j - 1, i]
        lanes = pl.ds(pl.multiple_of(k * rows, rows), rows)
        return mult_v[:, lanes] + aug_weight * (scale_v[:, lanes] * total - rhs_v[:, lanes])

    m_send[...] = new_mult(1 - core)
    n = len(pair)
    push(m_send, m_far)
    mult_out[own_rows, :] = new_mult(core)

    for copy in gathers:
        copy.wait()
    total_sum = sums_v[0, :, pl.ds(0, nv)]
    total = sums_v[0, :, pl.ds(nv, 128)]
    primal = sums_v[0, :, pl.ds(nv + 128, 128)]
    for i in range(1, n_scen):
        total_sum = total_sum + sums_v[i, :, pl.ds(0, nv)]
        total = total + sums_v[i, :, pl.ds(nv, 128)]
        primal = primal + sums_v[i, :, pl.ds(nv + 128, 128)]
    z_new = total_sum / total[:, :1]
    between = jnp.zeros_like(z_new)
    for i in range(n_scen):
        weight = sums_v[i, :, pl.ds(nv, 128)][:, :1]
        between = between + weight * (sums_v[i, :, pl.ds(0, nv)] / weight - z_new) ** 2
    primal = primal + jnp.sum(between, axis=1, keepdims=True)
    dual = jnp.sum((z_new - cons_v[0]) ** 2, axis=1, keepdims=True)
    norms_v[b, :, pl.ds(0, 128)] = primal
    norms_v[b, :, pl.ds(128, 128)] = jnp.broadcast_to(dual, (1, 128))
    norms = []
    for j in range(1, n_blk):
        copy = remote(norms_v.at[b], norms_v.at[b], n_send.at[j - 1], n_recv.at[j - 1], blk_peer(j))
        copy.start()
        norms.append(copy)
    z_out[...] = z_new
    pair[n].wait()
    mult_out[far_rows, :] = m_far[...]
    for copy in norms:
        copy.wait()
    primal = norms_v[0, :, pl.ds(0, 128)]
    dual = norms_v[0, :, pl.ds(128, 128)]
    for i in range(1, n_blk):
        primal = primal + norms_v[i, :, pl.ds(0, 128)]
        dual = dual + norms_v[i, :, pl.ds(128, 128)]
    width = nv * n_blk
    primal_out[...] = jnp.sqrt(primal / (total * width) + eps)
    dual_out[...] = penalty * jnp.sqrt(dual / width + eps)


def finish(sol, mult, z, primal, dual, ph, sol_out, mult_out, z_out, w_out, primal_out, dual_out):
    sol_out[...] = sol[...]
    mult_out[...] = mult[...]
    z_out[...] = z[...]
    w_out[...] = ph[...] + penalty * (sol[...] - z[...])
    primal_out[...] = primal[...]
    dual_out[...] = dual[...]


def solution(mesh):
    n_blk, n_scen = mesh.shape["blk"], mesh.shape["scen"]
    f32, bf16 = jnp.float32, jnp.bfloat16

    def per_device(cons_matrix, row_scale, rhs, cons_mult, cost, ph_mult, start, consensus, upper, prob):
        m, nv = cons_matrix.shape
        scen = cost.shape[0]
        half, rows = scen // 2, m // n_blk
        n_red = n_blk // 2
        any_spec = pl.BlockSpec(memory_space=pl.ANY)
        vmem = pl.BlockSpec(memory_space=pltpu.VMEM)
        dma = pltpu.SemaphoreType.DMA
        ends = pl.pallas_call(
            functools.partial(kernel, n_blk, n_scen),
            out_shape=(
                jax.ShapeDtypeStruct((scen, nv), f32),
                jax.ShapeDtypeStruct((scen, rows), f32),
                jax.ShapeDtypeStruct((1, nv), f32),
                jax.ShapeDtypeStruct((1, 128), f32),
                jax.ShapeDtypeStruct((1, 128), f32),
            ),
            in_specs=[any_spec] * 10,
            out_specs=[vmem] * 5,
            scratch_shapes=[
                pltpu.VMEM((2, n_blk, rows, nv), bf16),
                pltpu.VMEM((n_blk, 2, nv, rows), bf16),
                pltpu.VMEM((half, m), f32),
                pltpu.VMEM((half, m), f32),
                pltpu.VMEM((half, m), f32),
                pltpu.VMEM((n_blk, half, rows), f32),
                pltpu.VMEM((n_blk, half, rows), f32),
                pltpu.VMEM((2, half, nv), f32),
                pltpu.VMEM((scen, nv), f32),
                pltpu.VMEM((half, nv), f32),
                pltpu.VMEM((2, half, nv), f32),
                pltpu.VMEM((2, half, nv), bf16),
                pltpu.VMEM((2, half, nv), f32),
                pltpu.VMEM((2, 1, nv), f32),
                pltpu.VMEM((2, 1, nv), f32),
                pltpu.VMEM((1, scen), f32),
                pltpu.VMEM((n_blk, half, rows), f32),
                pltpu.VMEM((2, half, nv), f32),
                pltpu.VMEM((2, n_blk, half, rows), bf16),
                pltpu.VMEM((2, n_red - 1, n_blk, half, rows), bf16),
                pltpu.VMEM((n_red - 1, 2, half, rows), f32),
                pltpu.VMEM((half, nv), f32),
                pltpu.VMEM((half, rows), f32),
                pltpu.VMEM((half, rows), f32),
                pltpu.VMEM((n_scen, 1, nv + 256), f32),
                pltpu.VMEM((n_blk, 1, 256), f32),
                pltpu.VMEM((scen, nv), f32),
                pltpu.VMEM((n_blk, half, rows), f32),
                pltpu.VMEM((n_blk, half, rows), f32),
                dma((n_blk + 9,)),
                dma((2 * n_blk + 7,)),
                dma((2 * n_blk + 7,)),
                dma((2, n_red - 1, n_blk)),
                dma((2, n_red - 1, n_blk)),
                dma((n_red - 1, 2)),
                dma((n_red - 1, 2)),
                dma((n_scen - 1,)),
                dma((n_scen - 1,)),
                dma((n_blk - 1,)),
                dma((n_blk - 1,)),
            ],
            compiler_params=pltpu.CompilerParams(
                collective_id=0, has_side_effects=True, vmem_limit_bytes=67043328
            ),
        )(
            cons_matrix, row_scale, rhs, cons_mult, cost, ph_mult, start,
            consensus[None, :], upper[None, :], prob[None, :],
        )
        sol, mult_new, z_new, w_new, primal, dual = pl.pallas_call(
            finish,
            out_shape=tuple(
                jax.ShapeDtypeStruct(shape, f32)
                for shape in ((scen, nv), (scen, rows), (1, nv), (scen, nv), (1, 128), (1, 128))
            ),
            in_specs=[vmem] * 6,
            out_specs=[vmem] * 6,
        )(*ends, ph_mult)
        return sol, mult_new, z_new[0], w_new, primal[0, 0], dual[0, 0]

    in_specs = (
        P(None, "blk"),
        P("scen", None),
        P("scen", None),
        P("scen", None),
        P("scen", "blk"),
        P("scen", "blk"),
        P("scen", "blk"),
        P("blk"),
        P("blk"),
        P("scen"),
    )
    out_specs = (P("scen", "blk"), P("scen", "blk"), P("blk"), P("scen", "blk"), P(), P())
    return jax.shard_map(per_device, mesh=mesh, in_specs=in_specs, out_specs=out_specs, check_vma=False)
```
